32 devices in a mesh: fsdp: 32 (over z, y, x, core).
Axes of the slice: x: 2, y: 2, z: 4, core: 2. Of those that a mesh axis runs over, the one named last changes fastest.
Arguments:
- hidden_in: bfloat16 [32768, 768], P('fsdp'), may hold values from -6 to 6
- out_cotangent: bfloat16 [32768, 768], P('fsdp'), may hold values from -6 to 6
- segment_ids: int32 [512, 64], P('fsdp'), may hold values from 0 to 2, as said below
- partner_ids: int32 [1024], P('fsdp'), may hold values from 0 to 1023, as said below
- input_weight: bfloat16 [768, 2304], P('fsdp'), may hold values from -0.21875 to 0.21875
- query_bias: bfloat16 [768], P('fsdp'), may hold values from -3 to 3
- value_bias: bfloat16 [768], P('fsdp'), may hold values from -3 to 3
- output_weight: bfloat16 [768, 768], P('fsdp'), may hold values from -0.625 to 0.625
- output_bias: bfloat16 [768], P('fsdp'), may hold values from -3 to 3
- first_gain: bfloat16 [768], P('fsdp'), may hold values from 0.25 to 1.75
- first_shift: bfloat16 [768], P('fsdp'), may hold values from -1.75 to 1.75
- expand_weight: bfloat16 [768, 3072], P('fsdp'), may hold values from -0.21875 to 0.21875
- expand_bias: bfloat16 [3072], P('fsdp'), may hold values from -3 to 3
- reduce_weight: bfloat16 [3072, 768], P('fsdp'), may hold values from -0.15625 to 0.15625
- reduce_bias: bfloat16 [768], P('fsdp'), may hold values from -1.75 to 1.75
- second_gain: bfloat16 [768], P('fsdp'), may hold values from 0.25 to 1.75
- second_shift: bfloat16 [768], P('fsdp'), may hold values from -1.75 to 1.75
Outputs:
- sentence_loss: float32 [1024], P('fsdp')
- layer_output: bfloat16 [32768, 768], P('fsdp')
- input_grad: bfloat16 [32768, 768], P('fsdp')
- input_weight_grad: float32 [768, 2304], P('fsdp')
- query_bias_grad: float32 [768], P('fsdp')
- value_bias_grad: float32 [768], P('fsdp')
- output_weight_grad: float32 [768, 768], P('fsdp')
- output_bias_grad: float32 [768], P('fsdp')
- first_gain_grad: float32 [768], P('fsdp')
- first_shift_grad: float32 [768], P('fsdp')
- expand_weight_grad: float32 [768, 3072], P('fsdp')
- expand_bias_grad: float32 [3072], P('fsdp')
- reduce_weight_grad: float32 [3072, 768], P('fsdp')
- reduce_bias_grad: float32 [768], P('fsdp')
- second_gain_grad: float32 [768], P('fsdp')
- second_shift_grad: float32 [768], P('fsdp')
The draws below stay inside these ranges and needn't reach their ends.
Inputs may be any that keep to these rules, and one draw needn't show every extreme that they name: `segment_ids`: each row holds 2 sentences numbered 0 to 1 in order, each of 8 to 28 tokens, then a padding run numbered 2 that is never empty; ids never fall along a row. `partner_ids`: sentences come in pairs: the partner of the partner of i is i, and no sentence is its own partner.
All inputs are finite; a program needn't handle non-finite values.
Results may differ from the reference program's by a relative error of at most 0.014.
Values may be sent and summed in bfloat16 or wider, within the bound.
A program may use at most 192 MiB of HBM per device.

```python
import math
import jax
import jax.numpy as jnp
from jax import lax

D = 768
HEADS = 12
HEAD_DIM = 64
FF = 3072
SEQ = 64
SEG_ROW = 2
ROWS = 512
TOKENS = 32768
SENTS = 1024


def draw_segment_ids(key, part):
    lengths = jax.random.randint(key, (ROWS, SEG_ROW), SEQ // 8, SEQ * 7 // 16 + 1, dtype=jnp.int32)
    boundaries = jnp.cumsum(lengths, axis=1).astype(jnp.int32)
    position = jnp.arange(SEQ, dtype=jnp.int32)
    return jnp.sum((position[None, :, None] >= boundaries[:, None, :]).astype(jnp.int32), axis=2).astype(jnp.int32)


def draw_partner_ids(key, part):
    shuffled = jax.random.permutation(key, SENTS).astype(jnp.int32)
    firsts = shuffled[0::2]
    seconds = shuffled[1::2]
    partner = jnp.zeros((SENTS,), jnp.int32)
    return partner.at[firsts].set(seconds).at[seconds].set(firsts)


def block_levels(stream_key, extent, cuts, least, largest):
    factor_of = 1.0
    for dim, parts in cuts:
        heights = jax.random.uniform(jax.random.fold_in(jax.random.fold_in(stream_key, 6), dim), (parts,), jnp.float32, least / len(cuts), largest / len(cuts))
        factor_of = factor_of * jnp.repeat(jnp.exp(heights), extent[dim] // parts).reshape((-1,) + (1,) * (len(extent) - 1 - dim))
    return factor_of


def centred(rng, shape, deviation, reach, pieces=(), kind=jnp.bfloat16):
    values = jax.random.normal(rng, shape, jnp.float32) * deviation
    if len(pieces) > 0:
        values = block_levels(rng, shape, pieces, -0.22, 0.18) * values
    return jnp.clip(values, min=-reach, max=reach).astype(kind)


def setup_inputs(seed: int = 0) -> dict:
    keys = jax.random.split(jax.random.key(seed), 18)
    return {
        "hidden_in": centred(keys[0], (TOKENS, D), 1.0, 6.0, ((0, 32),)),
        "out_cotangent": centred(keys[1], (TOKENS, D), 1.0, 6.0, ((0, 32),)),
        "segment_ids": draw_segment_ids(jax.random.fold_in(keys[17], 71), 0),
        "partner_ids": draw_partner_ids(jax.random.fold_in(keys[17], 71), 0),
        "input_weight": centred(keys[4], (D, 3 * D), D ** -0.5, 0.21875, ((0, 32),)),
        "query_bias": centred(keys[5], (D,), 0.5, 3.0, ((0, 32),)),
        "value_bias": centred(keys[6], (D,), 0.5, 3.0, ((0, 32),)),
        "output_weight": centred(keys[7], (D, D), (D // 8) ** -0.5, 0.625, ((0, 32),)),
        "output_bias": centred(keys[8], (D,), 0.5, 3.0, ((0, 32),)),
        "first_gain": jnp.clip(1.0 + 0.15 * jax.random.normal(keys[9], (D,), jnp.float32), 0.25, 1.75).astype(jnp.bfloat16),
        "first_shift": centred(keys[10], (D,), 0.3, 1.75, ((0, 32),)),
        "expand_weight": centred(keys[11], (D, FF), D ** -0.5, 0.21875, ((0, 32),)),
        "expand_bias": centred(keys[12], (FF,), 0.5, 3.0, ((0, 32),)),
        "reduce_weight": centred(keys[13], (FF, D), (FF // 2) ** -0.5, 0.15625, ((0, 32),)),
        "reduce_bias": centred(keys[14], (D,), 0.3, 1.75, ((0, 32),)),
        "second_gain": jnp.clip(1.0 + 0.15 * jax.random.normal(keys[15], (D,), jnp.float32), 0.25, 1.75).astype(jnp.bfloat16),
        "second_shift": centred(keys[16], (D,), 0.3, 1.75, ((0, 32),)),
    }


@jax.custom_vjp
def low(v):
    return lax.optimization_barrier(v.astype(jnp.bfloat16)).astype(jnp.float32)

@jax.custom_vjp
def low_back(v):
    return v

def low_keep(v):
    return (low(v), None)

def low_pass(kept, grad):
    return (grad,)

def back_keep(v):
    return (v, None)

def back_low(kept, grad):
    return (low(grad),)
low.defvjp(low_keep, low_pass)
low_back.defvjp(back_keep, back_low)
scale_logit = 40.0
margin_value = 0.3
norm_eps = 1e-06
big_negative = -1e+30
highest = lax.Precision.HIGHEST

def precise_dot(left_side, right_side):
    return jnp.dot(left_side, right_side, precision=highest)

def layer_norm(values, norm_gain, norm_shift):
    center = values - lax.optimization_barrier(jnp.mean(values, axis=-1, keepdims=True))
    spread = lax.rsqrt(lax.optimization_barrier(jnp.mean(center * center, axis=-1, keepdims=True)) + norm_eps)
    return center * spread * norm_gain + norm_shift

def block_forward(params, hidden, segments):
    input_weight, query_bias, value_bias, output_weight, output_bias, first_gain, first_shift, expand_weight, expand_bias, reduce_weight, reduce_bias, second_gain, second_shift = params
    row_count = segments.shape[0]
    split_shape = (row_count, SEQ, HEADS, HEAD_DIM)
    projected = precise_dot(hidden, input_weight)
    queries = low(low_back(projected[:, :D] + query_bias))
    key_rows = low(low_back(projected[:, D:2 * D]))
    values = low(low_back(projected[:, 2 * D:] + value_bias))
    scores = jnp.einsum('rqhd,rkhd->rhqk', queries.reshape(split_shape), key_rows.reshape(split_shape), precision=highest)
    scores = low_back(scores * (1.0 / math.sqrt(HEAD_DIM)))
    allowed = (segments[:, :, None] == segments[:, None, :])[:, None, :, :]
    attention = jax.nn.softmax(jnp.where(allowed, scores, big_negative), axis=-1)
    mixed_rows = jnp.einsum('rhqk,rkhd->rqhd', low(attention), values.reshape(split_shape), precision=highest)
    attended = low(low_back(mixed_rows.reshape(-1, D)))
    branch = low_back(precise_dot(attended, output_weight) + output_bias)
    first_out = layer_norm(hidden + branch, first_gain, first_shift)
    expanded = low_back(precise_dot(low(first_out), expand_weight) + expand_bias)
    activated = low(jax.nn.gelu(expanded, approximate=False))
    reduced = low_back(precise_dot(activated, reduce_weight) + reduce_bias)
    second = layer_norm(first_out + reduced, second_gain, second_shift)
    valid_rows = (segments < SEG_ROW).astype(jnp.float32).reshape(-1, 1)
    output = second * valid_rows
    sentence = jnp.arange(SEG_ROW, dtype=jnp.int32)
    starts = lax.optimization_barrier(jnp.sum((segments[:, None, :] < sentence[None, :, None]).astype(jnp.int32), axis=2)).astype(jnp.int32)
    pooled = jnp.take_along_axis(output.reshape(row_count, SEQ, D), starts[:, :, None], axis=1).reshape(-1, D)
    unit_rows = low(pooled * lax.rsqrt(lax.optimization_barrier(jnp.mean(pooled * pooled, axis=-1, keepdims=True)) + norm_eps))
    return (output, unit_rows)

def sentence_losses(unit_rows, partners):
    total_count = unit_rows.shape[0]
    block_size = math.gcd(total_count, 256)
    columns = jnp.arange(total_count, dtype=jnp.int32)

    @jax.checkpoint
    def one_block(block_index):
        start = (block_index * block_size).astype(jnp.int32)
        rows_here = lax.dynamic_slice_in_dim(unit_rows, start, block_size, 0)
        partner_here = lax.dynamic_slice_in_dim(partners, start, block_size, 0)
        own_index = start + jnp.arange(block_size, dtype=jnp.int32)
        products = low_back(precise_dot(rows_here, unit_rows.T))
        is_partner = columns[None, :] == partner_here[:, None]
        logits = products * (scale_logit / D) - scale_logit * margin_value * is_partner.astype(jnp.float32)
        logits = jnp.where(columns[None, :] == own_index[:, None], big_negative, logits)
        totals = jax.nn.logsumexp(logits, axis=-1)
        picked = lax.optimization_barrier(jnp.sum(jnp.where(is_partner, logits, 0.0), axis=-1))
        return totals - picked
    block_losses = lax.map(one_block, jnp.arange(total_count // block_size, dtype=jnp.int32))
    return block_losses.reshape(total_count)

def reference(hidden_in, out_cotangent, segment_ids, partner_ids, input_weight, query_bias, value_bias, output_weight, output_bias, first_gain, first_shift, expand_weight, expand_bias, reduce_weight, reduce_bias, second_gain, second_shift):
    params = tuple((item.astype(jnp.float32) for item in (input_weight, query_bias, value_bias, output_weight, output_bias, first_gain, first_shift, expand_weight, expand_bias, reduce_weight, reduce_bias, second_gain, second_shift)))
    block_rows = math.gcd(ROWS, 64)
    blocks = ROWS // block_rows
    stacked_segments = segment_ids.reshape(blocks, block_rows, SEQ)

    def forward(hidden, weights):
        stacked = hidden.reshape(blocks, block_rows * SEQ, D)
        run_block = jax.checkpoint(lambda block_inputs: block_forward(weights, block_inputs[0], block_inputs[1]))
        outputs, unit_blocks = lax.map(run_block, (stacked, stacked_segments))
        losses = sentence_losses(unit_blocks.reshape(SENTS, D), partner_ids)
        return (losses, outputs.reshape(TOKENS, D))
    (losses, output), pullback = jax.vjp(forward, hidden_in.astype(jnp.float32), params)
    hidden_grad, weight_grads = pullback((jnp.ones_like(losses), out_cotangent.astype(jnp.float32)))
    return (losses, output.astype(jnp.bfloat16), hidden_grad.astype(jnp.bfloat16), weight_grads[0], weight_grads[1], weight_grads[2], weight_grads[3], weight_grads[4], weight_grads[5], weight_grads[6], weight_grads[7], weight_grads[8], weight_grads[9], weight_grads[10], weight_grads[11], weight_grads[12])
```

```python
import functools
import math

import jax
import jax.numpy as jnp
from jax import lax
from jax.experimental import pallas as pl
from jax.experimental.pallas import tpu as pltpu
from jax.sharding import PartitionSpec as P

MESH = pl.DeviceIdType.MESH


HEADS = 12
HEAD_DIM = 64
SEG_ROW = 2


scale_logit = 40.0
margin_value = 0.3
norm_eps = 1e-06
big_negative = -1e30


def norm_forward(values, norm_gain, norm_shift):
    center = values - jnp.mean(values, axis=-1, keepdims=True)
    spread = lax.rsqrt(jnp.mean(center * center, axis=-1, keepdims=True) + norm_eps)
    normed = center * spread
    return (normed * norm_gain.astype(jnp.float32) + norm_shift.astype(jnp.float32), normed, spread)


def norm_backward(grad_out, normed, spread, norm_gain):
    scaled = grad_out * norm_gain.astype(jnp.float32)
    grad_in = spread * (
        scaled
        - jnp.mean(scaled, axis=-1, keepdims=True)
        - normed * jnp.mean(scaled * normed, axis=-1, keepdims=True)
    )
    return (grad_in, jnp.sum(grad_out * normed, axis=0), jnp.sum(grad_out, axis=0))


def group_scores(queries, key_rows, labels):
    token_count = queries.shape[0]
    group_size = math.gcd(token_count, 128)
    split_shape = (token_count // group_size, group_size, HEADS, HEAD_DIM)
    scores = jnp.einsum(
        "gqhd,gkhd->ghqk",
        queries.reshape(split_shape),
        key_rows.reshape(split_shape),
        preferred_element_type=jnp.float32,
    ) * (1.0 / math.sqrt(HEAD_DIM))
    grouped = labels.reshape(-1, group_size)
    allowed = (grouped[:, :, None] == grouped[:, None, :])[:, None, :, :]
    return (scores, allowed, split_shape)


def attend(queries, key_rows, values, labels):
    scores, allowed, split_shape = group_scores(queries, key_rows, labels)
    masked = jnp.where(allowed, scores, big_negative)
    maxima = jnp.max(masked, axis=-1, keepdims=True)
    totals = maxima + jnp.log(jnp.sum(jnp.exp(masked - maxima), axis=-1, keepdims=True))
    attention = jnp.exp(masked - totals)
    mixed_rows = jnp.einsum(
        "ghqk,gkhd->gqhd",
        attention.astype(jnp.bfloat16),
        values.reshape(split_shape),
        preferred_element_type=jnp.float32,
    )
    return (mixed_rows.reshape(queries.shape), totals)


def attend_back(queries, key_rows, values, labels, totals, attended_grad):
    scores, allowed, split_shape = group_scores(queries, key_rows, labels)
    attention = jnp.where(allowed, jnp.exp(scores - totals), 0.0)
    upstream = attended_grad.reshape(split_shape)
    attention_grad = jnp.einsum(
        "gqhd,gkhd->ghqk", upstream, values.reshape(split_shape), preferred_element_type=jnp.float32
    )
    values_grad = jnp.einsum(
        "ghqk,gqhd->gkhd",
        attention.astype(jnp.bfloat16),
        upstream,
        preferred_element_type=jnp.float32,
    )
    scores_grad = (
        attention * (attention_grad - jnp.sum(attention * attention_grad, axis=-1, keepdims=True))
    ).astype(jnp.bfloat16)
    inverse_root = 1.0 / math.sqrt(HEAD_DIM)
    queries_grad = (
        jnp.einsum(
            "ghqk,gkhd->gqhd",
            scores_grad,
            key_rows.reshape(split_shape),
            preferred_element_type=jnp.float32,
        )
        * inverse_root
    )
    keys_grad = (
        jnp.einsum(
            "ghqk,gqhd->gkhd",
            scores_grad,
            queries.reshape(split_shape),
            preferred_element_type=jnp.float32,
        )
        * inverse_root
    )
    flat_shape = queries.shape
    return jnp.concatenate(
        [
            queries_grad.reshape(flat_shape).astype(jnp.bfloat16),
            keys_grad.reshape(flat_shape).astype(jnp.bfloat16),
            values_grad.reshape(flat_shape).astype(jnp.bfloat16),
        ],
        axis=1,
    )


def chip_grid(device_count):
    chips = device_count // 2
    side = max(1, round((chips / 2) ** (1.0 / 3.0)))
    return (side, side, chips // (side * side))


class Place:
    def __init__(self, device_count):
        self.sizes = chip_grid(device_count)
        self.strides = (1, self.sizes[0], self.sizes[0] * self.sizes[1])
        self.chips = device_count // 2
        self.me = lax.axis_index("fsdp")
        self.core = self.me % 2
        self.chip = self.me // 2
        self.partner = self.me + 1 - 2 * self.core
        self.at = [self.chip // stride % size for stride, size in zip(self.strides, self.sizes)]

    def ways(self, axis):
        if self.sizes[axis] == 1:
            return []
        if self.sizes[axis] == 2:
            return [(1 - 2 * self.at[axis], None)]
        return [(-1, self.at[axis] > 0), (1, self.at[axis] < self.sizes[axis] - 1)]

    def neighbour(self, axis, way):
        return self.me + 2 * self.strides[axis] * way

    def offset(self, axis, k):
        size, here = self.sizes[axis], self.at[axis]
        if size == 1:
            return 0 * k
        if size == 2:
            return k * (1 - 2 * here)
        least = jnp.minimum(here, size - 1 - here)
        near = (k + 1) // 2 * (1 - 2 * (k % 2))
        far = (k - least) * jnp.where(size - 1 - here > here, 1, -1)
        return jnp.where(k <= 2 * least, near, far)

    def item(self, k, order):
        ranks, offsets, left, chip = [], [], k, self.chip
        for axis in order:
            rank = left % self.sizes[axis]
            left = left // self.sizes[axis]
            offset = self.offset(axis, rank)
            ranks.append(rank)
            offsets.append(offset)
            chip = chip + offset * self.strides[axis]
        return chip, ranks, offsets

    def onward(self, order, ranks, offsets):
        found = []
        for stage, axis in enumerate(order):
            fresh = None
            for rank in ranks[stage + 1 :]:
                fresh = (rank == 0) if fresh is None else fresh & (rank == 0)
            for number, (way, there) in enumerate(self.ways(axis)):
                if there is None:
                    moving = ranks[stage] == 0
                else:
                    moving = there & ((ranks[stage] == 0) | (offsets[stage] * way < 0))
                condition = moving if fresh is None else fresh & moving
                found.append((stage, number, self.neighbour(axis, way), condition))
        return found

    def inward(self, order, ranks, offsets):
        found = []
        for stage, axis in enumerate(order):
            last = ranks[stage] > 0
            for rank in ranks[stage + 1 :]:
                last = last & (rank == 0)
            ways = self.ways(axis)
            for number, (way, there) in enumerate(ways):
                condition = last if there is None else last & (offsets[stage] * way > 0)
                found.append((stage, len(ways) - 1 - number, self.neighbour(axis, way), condition))
        return found

    def greet(self):
        barrier = pltpu.get_barrier_semaphore()
        pl.semaphore_signal(barrier, inc=1, device_id=(self.partner,), device_id_type=MESH)
        count = 1
        for axis in range(3):
            for way, there in self.ways(axis):

                def tell(way=way, axis=axis):
                    pl.semaphore_signal(
                        barrier,
                        inc=1,
                        device_id=(self.neighbour(axis, way),),
                        device_id_type=MESH,
                    )

                if there is None:
                    tell()
                    count = count + 1
                else:
                    pl.when(there)(tell)
                    count = count + there.astype(jnp.int32)
        pl.semaphore_wait(barrier, count)


def remote(source, target, send_sem, recv_sem, device):
    return pltpu.make_async_remote_copy(
        src_ref=source,
        dst_ref=target,
        send_sem=send_sem,
        recv_sem=recv_sem,
        device_id=(device,),
        device_id_type=MESH,
    )


def ways_of(sizes):
    return sum(0 if size == 1 else 1 if size == 2 else 2 for size in sizes)


def way_number(sizes, order, stage, number):
    return ways_of([sizes[axis] for axis in order[:stage]]) + number


def gather_kernel(device_count, groups, count, *refs):
    shards, wholes = refs[:count], refs[count : 2 * count]
    own_sem, near_sem, far_sem, send_sem = refs[2 * count :]
    place = Place(device_count)
    window = send_sem.shape[2]
    partner_way = send_sem.shape[1] - 1
    place.greet()
    for i in range(count):
        pltpu.make_async_copy(shards[i], wholes[i].at[place.me], own_sem.at[i]).start()

    def sends(k, order, i, first):
        chip, ranks, offsets = place.item(k, order)
        slot = wholes[i].at[2 * chip + place.core]
        source = shards[i] if first else slot
        slot_sem = lax.rem(k, window)
        found = []
        for stage, number, device, condition in place.onward(order, ranks, offsets):
            way = way_number(place.sizes, order, stage, number)
            found.append(
                (condition, remote(source, slot, send_sem.at[i, way, slot_sem], near_sem.at[i, chip], device))
            )
        found.append(
            (
                None,
                remote(
                    source,
                    slot,
                    send_sem.at[i, partner_way, slot_sem],
                    far_sem.at[i, chip],
                    place.partner,
                ),
            )
        )
        return slot, found

    def settle(k, order, i):
        for condition, copy in sends(k, order, i, False)[1]:
            if condition is None:
                copy.wait_send()
            else:
                pl.when(condition)(copy.wait_send)

    def advance(k, first):
        for order, members in groups:
            for i in members:
                if not first:
                    chip = place.item(k, order)[0]
                    slot = wholes[i].at[2 * chip + place.core]
                    remote(slot, slot, send_sem.at[i, 0, 0], near_sem.at[i, chip], place.partner).wait_recv()
                for condition, copy in sends(k, order, i, first)[1]:
                    if condition is None:
                        copy.start()
                    else:
                        pl.when(condition)(copy.start)

    advance(jnp.int32(0), True)

    def step(k, carry):
        if window < place.chips:

            @pl.when(k >= window)
            def _():
                for order, members in groups:
                    for i in members:
                        settle(k - window, order, i)

        advance(k, False)
        return carry

    lax.fori_loop(1, place.chips, step, 0)

    def finish(k, carry):
        for order, members in groups:
            for i in members:
                settle(k, order, i)
        return carry

    lax.fori_loop(place.chips - window, place.chips, finish, 0)

    def arrive(chip, carry):
        for i in range(count):
            slot = wholes[i].at[2 * chip + 1 - place.core]
            remote(slot, slot, send_sem.at[i, 0, 0], far_sem.at[i, chip], place.partner).wait_recv()
        return carry

    lax.fori_loop(0, place.chips, arrive, 0)
    for i in range(count):
        pltpu.make_async_copy(shards[i], wholes[i].at[place.me], own_sem.at[i]).wait()


def gather(device_count, shards, groups, collective_id, name):
    sizes = chip_grid(device_count)
    chips = device_count // 2
    count = len(shards)
    window = min(chips, 16)
    return pl.pallas_call(
        functools.partial(gather_kernel, device_count, groups, count),
        out_shape=tuple(jax.ShapeDtypeStruct((device_count,) + s.shape, s.dtype) for s in shards),
        in_specs=[pl.BlockSpec(memory_space=pltpu.VMEM)] * count,
        out_specs=tuple(pl.BlockSpec(memory_space=pl.ANY) for _ in shards),
        scratch_shapes=[
            pltpu.SemaphoreType.DMA((count,)),
            pltpu.SemaphoreType.DMA((count, chips)),
            pltpu.SemaphoreType.DMA((count, chips)),
            pltpu.SemaphoreType.DMA((count, ways_of(sizes) + 1, window)),
        ],
        compiler_params=pltpu.CompilerParams(collective_id=collective_id, has_side_effects=True),
        name=name,
    )(*shards)


def scatter_kernel(device_count, groups, count, *refs):
    parts, outs = refs[:count], refs[count : 2 * count]
    total, mate, inbox = (refs[(2 + j) * count : (3 + j) * count] for j in range(3))
    work = refs[5 * count : 6 * count]
    own_sem, near_sem, far_sem, send_sem, mate_sem = refs[6 * count :]
    place = Place(device_count)
    place.greet()

    def start(j, carry):
        k = place.chips - 1 - j
        for order, members in groups:
            chip, _, _ = place.item(k, order)
            for i in members:
                remote(
                    parts[i].at[2 * chip + 1 - place.core],
                    mate[i].at[chip],
                    mate_sem.at[i, chip],
                    far_sem.at[i, chip],
                    place.partner,
                ).start()
                pltpu.make_async_copy(
                    parts[i].at[2 * chip + place.core], total[i].at[chip], own_sem.at[i, chip]
                ).start()
        return carry

    lax.fori_loop(0, place.chips, start, 0)

    def box(i, order, stage, number, chip):
        spot, scale = 0, 1
        for axis in order[: stage + 1]:
            spot = spot + (chip // place.strides[axis] % place.sizes[axis]) * scale
            scale = scale * place.sizes[axis]
        first = 0
        for earlier in range(stage):
            first += boxes_at(place.sizes, order, earlier)
        return inbox[i].at[first + number * scale + spot], first + number * scale + spot

    def reduce_item(k, last):
        for order, members in groups:
            chip, ranks, offsets = place.item(k, order)
            for i in members:
                pltpu.make_async_copy(
                    parts[i].at[2 * chip + place.core], total[i].at[chip], own_sem.at[i, chip]
                ).wait()
                remote(
                    mate[i].at[chip], mate[i].at[chip], mate_sem.at[i, chip], far_sem.at[i, chip], place.partner
                ).wait_recv()
                work[i][...] = total[i][chip].astype(jnp.float32) + mate[i][chip].astype(jnp.float32)
                for stage, number, device, condition in place.onward(order, ranks, offsets):
                    slot, index = box(i, order, stage, number, chip)

                    def take(slot=slot, index=index, i=i):
                        remote(slot, slot, send_sem.at[i, 0], near_sem.at[i, index], place.partner).wait_recv()
                        work[i][...] = work[i][...] + inbox[i][index].astype(jnp.float32)

                    pl.when(condition)(take)
                if last:
                    outs[i][...] = work[i][...]
                else:
                    total[i][chip] = work[i][...].astype(total[i].dtype)
                    for stage, number, device, condition in place.inward(order, ranks, offsets):
                        slot, index = box(i, order, stage, number, chip)
                        copy = remote(
                            total[i].at[chip], slot, send_sem.at[i, chip], near_sem.at[i, index], device
                        )
                        pl.when(condition)(copy.start)

    def step(j, carry):
        reduce_item(place.chips - 1 - j, False)
        return carry

    lax.fori_loop(0, place.chips - 1, step, 0)
    reduce_item(jnp.int32(0), True)

    def finish(k, carry):
        for order, members in groups:
            chip, ranks, offsets = place.item(k, order)
            for i in members:
                remote(
                    mate[i].at[chip], mate[i].at[chip], mate_sem.at[i, chip], far_sem.at[i, chip], place.partner
                ).wait_send()

                @pl.when(k > 0)
                def _(i=i, chip=chip):
                    remote(
                        total[i].at[chip], total[i].at[chip], send_sem.at[i, chip], near_sem.at[i, 0], place.partner
                    ).wait_send()

        return carry

    lax.fori_loop(0, place.chips, finish, 0)


def boxes_at(sizes, order, stage):
    scale = 1
    for axis in order[: stage + 1]:
        scale *= sizes[axis]
    return scale * ways_of([sizes[order[stage]]])


def boxes_of(sizes, order):
    return sum(boxes_at(sizes, order, stage) for stage in range(3))


def scatter(device_count, parts, groups, collective_id, name):
    sizes = chip_grid(device_count)
    chips = device_count // 2
    count = len(parts)
    order_of = {i: order for order, members in groups for i in members}
    most = max(boxes_of(sizes, order) for order, _ in groups)
    vmem = pl.BlockSpec(memory_space=pltpu.VMEM)
    return pl.pallas_call(
        functools.partial(scatter_kernel, device_count, groups, count),
        out_shape=tuple(jax.ShapeDtypeStruct(p.shape[1:], jnp.float32) for p in parts),
        in_specs=[pl.BlockSpec(memory_space=pl.ANY)] * count,
        out_specs=(vmem,) * count,
        scratch_shapes=[pltpu.VMEM((chips,) + p.shape[1:], p.dtype) for p in parts]
        + [pltpu.VMEM((chips,) + p.shape[1:], p.dtype) for p in parts]
        + [
            pltpu.VMEM((boxes_of(sizes, order_of[i]),) + p.shape[1:], p.dtype)
            for i, p in enumerate(parts)
        ]
        + [pltpu.VMEM(p.shape[1:], jnp.float32) for p in parts]
        + [
            pltpu.SemaphoreType.DMA((count, chips)),
            pltpu.SemaphoreType.DMA((count, most)),
            pltpu.SemaphoreType.DMA((count, chips)),
            pltpu.SemaphoreType.DMA((count, chips)),
            pltpu.SemaphoreType.DMA((count, chips)),
        ],
        compiler_params=pltpu.CompilerParams(collective_id=collective_id, has_side_effects=True),
        name=name,
    )(*parts)
X, Y, Z = 0, 1, 2
SMALL_ROWS = 8
LANES = 128


def pack(vectors, ids):
    flat = jnp.concatenate([v.astype(jnp.float32) for v in vectors] + [ids.astype(jnp.float32)])
    return jnp.pad(flat, (0, SMALL_ROWS * LANES - flat.shape[0])).reshape(SMALL_ROWS, LANES)


def unpack(small, widths):
    flat = small.reshape(small.shape[0], -1)
    found, start = [], 0
    for width in widths:
        found.append(flat[:, start : start + width].reshape(-1))
        start += width
    return found


def pack_sums(sums, device_count):
    flat = jnp.concatenate([s.reshape(device_count, -1) for s in sums], axis=1)
    flat = jnp.pad(flat, ((0, 0), (0, SMALL_ROWS * LANES - flat.shape[1])))
    return flat.reshape(device_count, SMALL_ROWS, LANES)


class Links:
    def __init__(self, device_count, shard_rows):
        self.count = device_count
        self.tiled = shard_rows % 8 == 0 and device_count // 2 <= 16

    def spread(self, shards, groups, collective_id, name):
        if self.tiled:
            return gather(self.count, shards, groups, collective_id, name)
        return [lax.all_gather(s, "fsdp") for s in shards]

    def sum_up(self, parts, groups, collective_id, name):
        if self.tiled:
            return scatter(self.count, parts, groups, collective_id, name)
        return [
            lax.psum_scatter(p.astype(jnp.float32), "fsdp", scatter_dimension=0, tiled=False) for p in parts
        ]


def on_device(
    device_count,
    hidden_in,
    out_cotangent,
    segment_ids,
    partner_ids,
    input_weight,
    query_bias,
    value_bias,
    output_weight,
    output_bias,
    first_gain,
    first_shift,
    expand_weight,
    expand_bias,
    reduce_weight,
    reduce_bias,
    second_gain,
    second_shift,
):
    device_rank = lax.axis_index("fsdp")
    token_count, model_width = hidden_in.shape
    row_count, seq_len = segment_ids.shape
    hidden_width = expand_weight.shape[1]
    contract_rows = (((0,), (0,)), ((), ()))
    contract_cols = (((1,), (1,)), ((), ()))
    links = Links(device_count, input_weight.shape[0])
    vectors = (
        query_bias,
        value_bias,
        output_bias,
        first_gain,
        first_shift,
        reduce_bias,
        second_gain,
        second_shift,
        expand_bias,
    )
    widths = [v.shape[0] for v in vectors]
    orders = ((X, Y, Z), (Z, X, Y), (Z, Y, X))
    groups = ((orders[0], (0,)), (orders[1], (1, 2)), (orders[2], (3, 4)))
    spread = links.spread(
        (input_weight, output_weight, expand_weight, reduce_weight, pack(vectors, partner_ids)),
        groups,
        1,
        "gather_weights",
    )
    input_all = spread[0].reshape(model_width, -1)
    output_all = spread[1].reshape(model_width, -1)
    expand_all = spread[2].reshape(model_width, -1)
    reduce_all = spread[3].reshape(hidden_width, -1)
    small = unpack(spread[4], widths + [partner_ids.shape[0]])
    query_add, value_add, output_add, gain_one, shift_one, reduce_add, gain_two, shift_two, expand_add = small[:9]
    partners_all = small[9].astype(jnp.int32)

    projected = jnp.dot(hidden_in, input_all, preferred_element_type=jnp.float32)
    queries = (projected[:, :model_width] + query_add).astype(jnp.bfloat16)
    key_rows = projected[:, model_width : 2 * model_width].astype(jnp.bfloat16)
    values = (projected[:, 2 * model_width :] + value_add).astype(jnp.bfloat16)
    flat_ids = segment_ids.reshape(-1)
    row_of = jnp.arange(token_count, dtype=jnp.int32) // seq_len
    labels = row_of * (SEG_ROW + 1) + flat_ids
    mixed_rows, totals = attend(queries, key_rows, values, labels)
    attended = mixed_rows.astype(jnp.bfloat16)
    branch = jnp.dot(attended, output_all, preferred_element_type=jnp.float32) + output_add
    first_out, first_normed, first_spread = norm_forward(
        hidden_in.astype(jnp.float32) + branch, gain_one, shift_one
    )
    first_low = first_out.astype(jnp.bfloat16)
    expanded = jnp.dot(first_low, expand_all, preferred_element_type=jnp.float32) + expand_add
    activated = jax.nn.gelu(expanded, approximate=False).astype(jnp.bfloat16)
    reduced = jnp.dot(activated, reduce_all, preferred_element_type=jnp.float32) + reduce_add
    second, second_normed, second_spread = norm_forward(first_out + reduced, gain_two, shift_two)
    valid_rows = (flat_ids < SEG_ROW).astype(jnp.float32)[:, None]
    output = second * valid_rows
    layer_output = output.astype(jnp.bfloat16)
    sentence = jnp.arange(SEG_ROW, dtype=jnp.int32)
    starts = jnp.sum((segment_ids[:, None, :] < sentence[None, :, None]).astype(jnp.int32), axis=2)
    pooled = jnp.take_along_axis(
        output.reshape(row_count, seq_len, model_width), starts[:, :, None], axis=1
    ).reshape(-1, model_width)
    inverse = lax.rsqrt(jnp.mean(pooled * pooled, axis=-1, keepdims=True) + norm_eps)
    unit_rows = (pooled * inverse).astype(jnp.bfloat16)
    third = model_width // 3
    unit_parts = links.spread(
        tuple(unit_rows[:, i * third : (i + 1) * third] for i in range(3)),
        tuple((order, (i,)) for i, order in enumerate(orders)),
        2,
        "gather_units",
    )
    all_units = jnp.concatenate([p.reshape(-1, third) for p in unit_parts], axis=1)
    local_count = unit_rows.shape[0]
    total_count = all_units.shape[0]
    columns = jnp.arange(total_count, dtype=jnp.int32)

    def logits_of(rows, row_index, partners):
        products = lax.dot_general(rows, all_units, contract_cols, preferred_element_type=jnp.float32)
        is_partner = columns[None, :] == partners[:, None]
        logits = products * (scale_logit / model_width) - scale_logit * margin_value * is_partner.astype(
            jnp.float32
        )
        return jnp.where(columns[None, :] == row_index[:, None], big_negative, logits), is_partner

    def log_sum(logits):
        maxima = jnp.max(logits, axis=-1)
        return maxima + jnp.log(jnp.sum(jnp.exp(logits - maxima[:, None]), axis=-1))

    own_index = device_rank * local_count + jnp.arange(local_count, dtype=jnp.int32)
    logits, is_partner = logits_of(unit_rows, own_index, partner_ids)
    row_total = log_sum(logits)
    if total_count <= 2048:
        every_total = log_sum(logits_of(all_units, columns, partners_all)[0])
    else:
        every_total = lax.all_gather(row_total, "fsdp", axis=0, tiled=True)
    sentence_loss = row_total - jnp.sum(jnp.where(is_partner, logits, 0.0), axis=-1)
    partner_float = is_partner.astype(jnp.float32)
    slope = scale_logit / model_width
    row_part = ((jnp.exp(logits - row_total[:, None]) - partner_float) * slope).astype(jnp.bfloat16)
    column_part = ((jnp.exp(logits - every_total[None, :]) - partner_float) * slope).astype(jnp.bfloat16)
    unit_grad = jnp.dot(row_part, all_units, preferred_element_type=jnp.float32) + jnp.dot(
        column_part, all_units, preferred_element_type=jnp.float32
    )
    pooled_grad = inverse * unit_grad - inverse * inverse * inverse * pooled * jnp.mean(
        unit_grad * pooled, axis=-1, keepdims=True
    )
    one_hot = (jnp.arange(seq_len, dtype=jnp.int32)[None, None, :] == starts[:, :, None]).astype(jnp.float32)
    placed = jnp.einsum(
        "rst,rsd->rtd",
        one_hot,
        pooled_grad.reshape(row_count, SEG_ROW, model_width),
        precision=lax.Precision.HIGHEST,
    ).reshape(-1, model_width)
    output_grad = (out_cotangent.astype(jnp.float32) + placed) * valid_rows
    second_in_grad, second_gain_grad, second_shift_grad = norm_backward(
        output_grad, second_normed, second_spread, gain_two
    )
    reduced_grad = second_in_grad.astype(jnp.bfloat16)
    reduce_weight_grad = lax.dot_general(
        activated, reduced_grad, contract_rows, preferred_element_type=jnp.float32
    )
    reduce_bias_grad = jnp.sum(reduced_grad, axis=0, dtype=jnp.float32)
    activated_grad = lax.dot_general(
        reduced_grad, reduce_all, contract_cols, preferred_element_type=jnp.float32
    )
    _, gelu_pullback = jax.vjp(lambda inner_value: jax.nn.gelu(inner_value, approximate=False), expanded)
    expanded_grad = gelu_pullback(activated_grad)[0].astype(jnp.bfloat16)
    expand_weight_grad = lax.dot_general(
        first_low, expanded_grad, contract_rows, preferred_element_type=jnp.float32
    )
    expand_bias_grad = jnp.sum(expanded_grad, axis=0, dtype=jnp.float32)
    first_grad = second_in_grad + lax.dot_general(
        expanded_grad, expand_all, contract_cols, preferred_element_type=jnp.float32
    )
    first_in_grad, first_gain_grad, first_shift_grad = norm_backward(
        first_grad, first_normed, first_spread, gain_one
    )
    branch_grad = first_in_grad.astype(jnp.bfloat16)
    output_weight_grad = lax.dot_general(
        attended, branch_grad, contract_rows, preferred_element_type=jnp.float32
    )
    output_bias_grad = jnp.sum(branch_grad, axis=0, dtype=jnp.float32)
    attended_grad = lax.dot_general(
        branch_grad, output_all, contract_cols, preferred_element_type=jnp.float32
    ).astype(jnp.bfloat16)
    projected_grad = attend_back(queries, key_rows, values, labels, totals, attended_grad)
    input_weight_grad = lax.dot_general(
        hidden_in, projected_grad, contract_rows, preferred_element_type=jnp.float32
    )
    query_bias_grad = jnp.sum(projected_grad[:, :model_width], axis=0, dtype=jnp.float32)
    value_bias_grad = jnp.sum(projected_grad[:, 2 * model_width :], axis=0, dtype=jnp.float32)
    input_grad = (
        first_in_grad
        + lax.dot_general(projected_grad, input_all, contract_cols, preferred_element_type=jnp.float32)
    ).astype(jnp.bfloat16)
    sums = (
        query_bias_grad,
        value_bias_grad,
        output_bias_grad,
        first_gain_grad,
        first_shift_grad,
        reduce_bias_grad,
        second_gain_grad,
        second_shift_grad,
        expand_bias_grad,
    )

    def blocks(weight_grad):
        return weight_grad.astype(jnp.bfloat16).reshape(device_count, -1, weight_grad.shape[1])

    owned = links.sum_up(
        (
            blocks(input_weight_grad),
            blocks(output_weight_grad),
            blocks(expand_weight_grad),
            blocks(reduce_weight_grad),
            pack_sums(sums, device_count),
        ),
        groups,
        3,
        "scatter_grads",
    )
    small_grads = unpack(owned[4][None], widths)
    return (
        sentence_loss,
        layer_output,
        input_grad,
        owned[0],
        small_grads[0],
        small_grads[1],
        owned[1],
        small_grads[2],
        small_grads[3],
        small_grads[4],
        owned[2],
        small_grads[8],
        owned[3],
        small_grads[5],
        small_grads[6],
        small_grads[7],
    )


def solution(mesh):
    in_specs = (
        P("fsdp", None),
        P("fsdp", None),
        P("fsdp", None),
        P("fsdp"),
        P("fsdp", None),
        P("fsdp"),
        P("fsdp"),
        P("fsdp", None),
        P("fsdp"),
        P("fsdp"),
        P("fsdp"),
        P("fsdp", None),
        P("fsdp"),
        P("fsdp", None),
        P("fsdp"),
        P("fsdp"),
        P("fsdp"),
    )
    out_specs = (
        P("fsdp"),
        P("fsdp", None),
        P("fsdp", None),
        P("fsdp", None),
        P("fsdp"),
        P("fsdp"),
        P("fsdp", None),
        P("fsdp"),
        P("fsdp"),
        P("fsdp"),
        P("fsdp", None),
        P("fsdp"),
        P("fsdp", None),
        P("fsdp"),
        P("fsdp"),
        P("fsdp"),
    )
    return jax.shard_map(
        functools.partial(on_device, mesh.shape["fsdp"]), mesh=mesh, in_specs=in_specs, out_specs=out_specs, check_vma=False
    )
```
